16 devices in a mesh: dp: 2 (over y, z), tp: 8 (over x, core).
Axes of the slice: x: 4, y: 2, z: 1, core: 2. Of those that a mesh axis runs over, the one named last changes fastest.
The devices are a block of a 4x4x8 slice.
Arguments:
- x_in: bfloat16 [32, 512, 2560], P('dp', 'tp'), parts along dimension 0
- rope_angle: float32 [512, 16], replicated
- ln_gain: float32 [2560], replicated
- ln_bias: float32 [2560], replicated
- w_q: bfloat16 [2560, 2560], P(None, 'tp')
- b_q: float32 [32, 80], P('tp')
- w_k: bfloat16 [2560, 2560], P(None, 'tp')
- b_k: float32 [32, 80], P('tp')
- w_v: bfloat16 [2560, 2560], P(None, 'tp')
- b_v: float32 [32, 80], P('tp')
- w_o: bfloat16 [2560, 2560], P('tp')
- b_o: float32 [2560], replicated
- w_up: bfloat16 [2560, 10240], P(None, 'tp')
- b_up: float32 [10240], P('tp')
- w_down: bfloat16 [10240, 2560], P('tp')
- b_down: float32 [2560], replicated
- dy_out: bfloat16 [32, 512, 2560], P('dp', 'tp'), parts along dimension 0
Outputs:
- output 1: bfloat16 [32, 512, 2560], P('dp', 'tp'), parts along dimension 0
- output 2: float32 [32, 512, 2560], P('dp', 'tp'), parts along dimension 0
- output 3: float32 [5120], P('dp'), parts along dimension 0
- output 4: float32 [5120], P('dp'), parts along dimension 0
- output 5: float32 [5120, 2560], P('dp', 'tp'), parts along dimension 0
- output 6: float32 [64, 80], P(('dp', 'tp')), parts along dimension 0
- output 7: float32 [5120, 2560], P('dp', 'tp'), parts along dimension 0
- output 8: float32 [64, 80], P(('dp', 'tp')), parts along dimension 0
- output 9: float32 [5120, 2560], P('dp', 'tp'), parts along dimension 0
- output 10: float32 [64, 80], P(('dp', 'tp')), parts along dimension 0
- output 11: float32 [5120, 2560], P(('dp', 'tp')), parts along dimension 0
- output 12: float32 [5120], P('dp'), parts along dimension 0
- output 13: float32 [5120, 10240], P('dp', 'tp'), parts along dimension 0
- output 14: float32 [20480], P(('dp', 'tp')), parts along dimension 0
- output 15: float32 [20480, 2560], P(('dp', 'tp')), parts along dimension 0
- output 16: float32 [5120], P('dp'), parts along dimension 0
There are 2 independent parts. The reference program is written for one: setup_inputs(seed, part) draws one part's arguments, and reference() takes and returns one part's arrays. A program takes and returns all parts, laid end to end along the dimension named above; an argument that names none is the same for every part.
All inputs are finite; a program needn't handle non-finite values.
Results may differ from the reference program's by a relative error of at most 0.02.
Values are sent between devices in bfloat16 or wider.
A program may use at most 768 MiB of HBM per device.

```python
import jax
import jax.numpy as jnp
from jax import lax

NUM_SEQS = 16
SEQ_LEN = 512
MODEL_DIM = 2560
NUM_HEADS = 32
ROT_DIM = 32
FFN_DIM = 10240

HEAD_DIM = MODEL_DIM // NUM_HEADS
HALF_ROT = ROT_DIM // 2
LN_EPS = 1e-5
ROPE_BASE = 10000.0


def setup_inputs(seed: int = 0, part: int = 0) -> dict:
    base_key = jax.random.key(seed)
    shared_keys = jax.random.split(base_key, 15)
    part_keys = jax.random.split(jax.random.fold_in(base_key, part), 3)

    def normal(rng_key, arr_shape):
        return jax.random.normal(rng_key, arr_shape, jnp.float32)

    def weight(rng_key, fan_in, fan_out):
        return (normal(rng_key, (fan_in, fan_out)) * fan_in ** -0.5).astype(jnp.bfloat16)

    pos_gaps = jax.random.randint(shared_keys[0], (SEQ_LEN,), 1, 5)
    positions = jnp.cumsum(pos_gaps).astype(jnp.float32)
    inv_freq = ROPE_BASE ** (-jnp.arange(0, ROT_DIM, 2).astype(jnp.float32) / ROT_DIM)
    tok_scale = jnp.exp(0.5 * normal(part_keys[0], (NUM_SEQS, SEQ_LEN, 1)))
    act_shape = (NUM_SEQS, SEQ_LEN, MODEL_DIM)
    head_shape = (NUM_HEADS, HEAD_DIM)
    return {
        'x_in': (normal(part_keys[1], act_shape) * tok_scale).astype(jnp.bfloat16),
        'rope_angle': positions[:, None] * inv_freq[None, :],
        'ln_gain': 1.0 + 0.2 * normal(shared_keys[1], (MODEL_DIM,)),
        'ln_bias': 0.5 * normal(shared_keys[2], (MODEL_DIM,)),
        'w_q': weight(shared_keys[3], MODEL_DIM, MODEL_DIM),
        'b_q': 0.5 * normal(shared_keys[4], head_shape),
        'w_k': weight(shared_keys[5], MODEL_DIM, MODEL_DIM),
        'b_k': 0.5 * normal(shared_keys[6], head_shape),
        'w_v': weight(shared_keys[7], MODEL_DIM, MODEL_DIM),
        'b_v': 0.5 * normal(shared_keys[8], head_shape),
        'w_o': weight(shared_keys[9], MODEL_DIM, MODEL_DIM),
        'b_o': 0.5 * normal(shared_keys[10], (MODEL_DIM,)),
        'w_up': weight(shared_keys[11], MODEL_DIM, FFN_DIM),
        'b_up': 0.5 * normal(shared_keys[12], (FFN_DIM,)),
        'w_down': weight(shared_keys[13], FFN_DIM, MODEL_DIM),
        'b_down': 0.5 * normal(shared_keys[14], (MODEL_DIM,)),
        'dy_out': normal(part_keys[2], act_shape).astype(jnp.bfloat16),
    }


def to_bf16(t):
    return t.astype(jnp.bfloat16).astype(jnp.float32)


def rope_rotate(t, cos_t, sin_t):
    t_rot = t[..., :ROT_DIM]
    turned = jnp.concatenate([-t_rot[..., HALF_ROT:], t_rot[..., :HALF_ROT]], axis=-1)
    return jnp.concatenate([t_rot * cos_t + turned * sin_t, t[..., ROT_DIM:]], axis=-1)


def head_attention(triple):
    q_head, k_head, v_head = triple
    seq_pos = jnp.arange(SEQ_LEN)
    scores = jnp.einsum('bqd,bkd->bqk', q_head, k_head) * HEAD_DIM ** -0.5
    scores = jnp.where(seq_pos[:, None] >= seq_pos[None, :], scores, -1e30)
    prob_mat = to_bf16(jax.nn.softmax(scores, axis=-1))
    return to_bf16(jnp.einsum('bqk,bkd->bqd', prob_mat, v_head))


def layer_forward(x_f, ln_gain, ln_bias, w_q, b_q, w_k, b_k, w_v, b_v, w_o, b_o, w_up, b_up, w_down, b_down, cos_t, sin_t):
    centered = x_f - jnp.mean(x_f, axis=-1, keepdims=True)
    inv_std = lax.rsqrt(jnp.mean(centered * centered, axis=-1, keepdims=True) + LN_EPS)
    h_flat = to_bf16(centered * inv_std * ln_gain + ln_bias).reshape(NUM_SEQS * SEQ_LEN, MODEL_DIM)

    def project(w_mat, b_vec):
        linear = jnp.dot(h_flat, w_mat, preferred_element_type=jnp.float32)
        return to_bf16(linear.reshape(NUM_SEQS, SEQ_LEN, NUM_HEADS, HEAD_DIM) + b_vec)

    q_r = to_bf16(rope_rotate(project(w_q, b_q), cos_t, sin_t))
    k_r = to_bf16(rope_rotate(project(w_k, b_k), cos_t, sin_t))
    v_p = project(w_v, b_v)
    heads_first = (jnp.transpose(q_r, (2, 0, 1, 3)), jnp.transpose(k_r, (2, 0, 1, 3)), jnp.transpose(v_p, (2, 0, 1, 3)))
    context = lax.map(jax.checkpoint(head_attention), heads_first)
    ctx_flat = jnp.transpose(context, (1, 2, 0, 3)).reshape(NUM_SEQS * SEQ_LEN, MODEL_DIM)
    act_bf = to_bf16(jax.nn.gelu(jnp.dot(h_flat, w_up, preferred_element_type=jnp.float32) + b_up, approximate=True))
    y_flat = (x_f.reshape(NUM_SEQS * SEQ_LEN, MODEL_DIM)
              + jnp.dot(ctx_flat, w_o, preferred_element_type=jnp.float32)
              + jnp.dot(act_bf, w_down, preferred_element_type=jnp.float32)
              + b_o + b_down)
    return y_flat.reshape(NUM_SEQS, SEQ_LEN, MODEL_DIM)


def reference(x_in, rope_angle, ln_gain, ln_bias, w_q, b_q, w_k, b_k, w_v, b_v, w_o, b_o, w_up, b_up, w_down, b_down, dy_out):
    angle_pair = jnp.concatenate([rope_angle, rope_angle], axis=-1)[None, :, None, :]
    cos_t = jnp.cos(angle_pair)
    sin_t = jnp.sin(angle_pair)
    primals = (x_in.astype(jnp.float32), ln_gain, ln_bias,
               w_q.astype(jnp.float32), b_q, w_k.astype(jnp.float32), b_k,
               w_v.astype(jnp.float32), b_v, w_o.astype(jnp.float32), b_o,
               w_up.astype(jnp.float32), b_up, w_down.astype(jnp.float32), b_down)
    y_f, pull_back = jax.vjp(lambda *values_in: layer_forward(*values_in, cos_t, sin_t), *primals)
    all_grads = pull_back(dy_out.astype(jnp.float32))
    return (y_f.astype(jnp.bfloat16), all_grads[0], all_grads[1], all_grads[2], all_grads[3],
            all_grads[4], all_grads[5], all_grads[6], all_grads[7], all_grads[8], all_grads[9],
            all_grads[10], all_grads[11], all_grads[12], all_grads[13], all_grads[14])
```

```python
import functools

import jax
import jax.numpy as jnp
from jax import lax
from jax.experimental import pallas as pl
from jax.experimental.pallas import tpu as pltpu
from jax.sharding import PartitionSpec as P

LN_EPS = 1e-5
CHUNK_PARTS = (1, 1, 1, 1)
LOG2E = 1.4426950408889634
GELU_A, GELU_B = 0.7978845608028654, 0.044715
F32, BF16 = jnp.float32, jnp.bfloat16


def dot_t(a, b, dims):
    return lax.dot_general(a, b, (dims, ((), ())), preferred_element_type=F32)


def call(kernel, name, grid, ins, outs, flops, full=()):
    arrays, specs = [a for a, _ in ins], [s for _, s in ins]
    first = len(outs) - len(full)
    aliases = {}
    for i, prev in enumerate(full):
        if prev is not None:
            aliases[len(arrays)] = first + i
            arrays.append(prev)
            specs.append(pl.BlockSpec(memory_space=pl.ANY))
    n_in = len(ins)

    def body(*refs):
        kernel(*refs[:n_in], *refs[len(arrays):])

    moved = sum(a.size * a.dtype.itemsize for a, _ in ins)
    return pl.pallas_call(
        body, grid=grid, in_specs=specs, out_specs=[s for _, _, s in outs],
        out_shape=[jax.ShapeDtypeStruct(s, d) for s, d, _ in outs], input_output_aliases=aliases,
        cost_estimate=pl.CostEstimate(flops=flops, bytes_accessed=moved, transcendentals=0), name=name)(*arrays)


def attn_kernel(heads, head_dim, half_rot, qkv_ref, dctx_ref, cos_ref, sin_ref, ctx_ref, dqkv_ref, bsum_ref, ctx_all_ref, dqkv_all_ref):
    seq_len = qkv_ref.shape[1]
    half = seq_len // 2
    width = heads * head_dim
    scale = head_dim ** -0.5
    cos_t, sin_t = cos_ref[...], sin_ref[...]
    mask = (lax.broadcasted_iota(jnp.int32, (half, half), 0) <= lax.broadcasted_iota(jnp.int32, (half, half), 1))

    def rope(t, sin_s):
        turned = jnp.concatenate([-t[:, half_rot:2 * half_rot], t[:, :half_rot], t[:, 2 * half_rot:]], axis=-1)
        return t * cos_t + turned * sin_s

    @pl.when(pl.program_id(0) == 0)
    def _():
        bsum_ref[...] = jnp.zeros_like(bsum_ref)

    for i in range(heads):
        cols = [slice(w * width + i * head_dim, w * width + (i + 1) * head_dim) for w in range(3)]
        own = cols[0]
        q = rope(qkv_ref[0, :, cols[0]].astype(F32), sin_t).astype(BF16)
        k = rope(qkv_ref[0, :, cols[1]].astype(F32), sin_t).astype(BF16)
        v = qkv_ref[0, :, cols[2]]
        d_ctx = dctx_ref[0, :, own]
        k_t, v_t = k.T, v.T
        ctx_t, dq_t, dk, dv = [], [], [], []
        for b in range(2):
            rows = slice(b * half, (b + 1) * half)
            keys = (b + 1) * half
            s = dot_t(k[:keys], q[rows], ((1,), (1,)))
            diag = jnp.where(mask, s[b * half:], -1e30)
            s = diag if b == 0 else jnp.concatenate([s[:half], diag], axis=0)
            e = jnp.exp2((s - jnp.max(s, axis=0, keepdims=True)) * (scale * LOG2E))
            prob = e * (1.0 / jnp.sum(e, axis=0, keepdims=True))
            prob_bf = prob.astype(BF16)
            ctx_t.append(dot_t(v_t[:, :keys], prob_bf, ((1,), (0,))).astype(BF16))
            d_prob = dot_t(v[:keys], d_ctx[rows], ((1,), (1,)))
            d_score = (prob * (d_prob - jnp.sum(d_prob * prob, axis=0, keepdims=True)) * scale).astype(BF16)
            dq_t.append(dot_t(k_t[:, :keys], d_score, ((1,), (0,))))
            dk.append(dot_t(d_score, q[rows], ((1,), (0,))))
            dv.append(dot_t(prob_bf, d_ctx[rows], ((1,), (0,))))
        ctx = jnp.concatenate(ctx_t, axis=1).T
        ctx_ref[0, :, own] = ctx
        ctx_all_ref[:, own] = ctx
        d_q = rope(jnp.concatenate(dq_t, axis=1).T, -sin_t)
        d_k = rope(jnp.concatenate([dk[0] + dk[1][:half], dk[1][half:]], axis=0), -sin_t)
        d_v = jnp.concatenate([dv[0] + dv[1][:half], dv[1][half:]], axis=0)
        for d_p, col in zip((d_q, d_k, d_v), cols):
            dqkv_ref[0, :, col] = d_p.astype(BF16)
            dqkv_all_ref[:, col] = d_p.astype(BF16)
            bsum_ref[:, col] += jnp.sum(d_p, axis=0, keepdims=True)


def attention(qkv, d_ctx, cos_full, sin_full, heads, head_dim, half_rot, seq0, total, full):
    n_seq, seq_len, width3 = qkv.shape
    width = heads * head_dim
    tab = pl.BlockSpec((seq_len, head_dim), lambda i: (0, 0))
    block = lambda w: pl.BlockSpec((1, seq_len, w), lambda i: (i, 0, 0))
    rows = lambda w: pl.BlockSpec((seq_len, w), lambda i: (i + seq0, 0))
    return call(functools.partial(attn_kernel, heads, head_dim, half_rot), "attention", (n_seq,),
                [(qkv, block(width3)), (d_ctx, block(width)), (cos_full, tab), (sin_full, tab)],
                [((n_seq, seq_len, width), BF16, block(width)), ((n_seq, seq_len, width3), BF16, block(width3)),
                 ((1, width3), F32, pl.BlockSpec((1, width3), lambda i: (0, 0))),
                 ((total, width), BF16, rows(width)), ((total, width3), BF16, rows(width3))],
                n_seq * heads * 4 * 2 * seq_len * seq_len * 256, full)


def const(arr):
    return (arr, pl.BlockSpec(arr.shape, lambda i: (0, 0)))


def normalize(x):
    x_f = x.astype(F32)
    centered = x_f - jnp.mean(x_f, axis=-1, keepdims=True)
    inv_std = lax.rsqrt(jnp.mean(centered * centered, axis=-1, keepdims=True) + LN_EPS)
    return centered * inv_std, inv_std


def ln_fwd_kernel(x_ref, gain_ref, bias_ref, h_ref):
    normed, _ = normalize(x_ref[0])
    h_ref[0] = (normed * gain_ref[...] + bias_ref[...]).astype(BF16)


def ln_bwd_kernel(x_ref, dy_ref, dh_ref, gain_ref, sums_ref, dx_ref):
    @pl.when(pl.program_id(0) == 0)
    def _():
        sums_ref[...] = jnp.zeros_like(sums_ref)

    normed, inv_std = normalize(x_ref[0])
    d_h, dy = dh_ref[0].astype(F32), dy_ref[0].astype(F32)
    d_norm = d_h * gain_ref[...]
    sums_ref[0:1] += jnp.sum(d_h * normed, axis=0, keepdims=True)
    sums_ref[1:2] += jnp.sum(d_h, axis=0, keepdims=True)
    sums_ref[2:3] += jnp.sum(dy, axis=0, keepdims=True)
    dx_ref[0] = dy + inv_std * (d_norm - jnp.mean(d_norm, axis=-1, keepdims=True)
                                - normed * jnp.mean(d_norm * normed, axis=-1, keepdims=True))


def residual_kernel(x_ref, part_ref, bo_ref, bdown_ref, y_ref):
    y_ref[0] = (x_ref[0].astype(F32) + part_ref[0].astype(F32) + bo_ref[...] + bdown_ref[...]).astype(BF16)


def front_h_kernel(tile, h_ref, wqkv_ref, bqkv_ref, wup_ref, bup_ref, qkv_ref, act_ref, slope_ref, act_all_ref, h_all_ref):
    h = h_ref[...]
    h_all_ref[...] = h
    for j in range(act_ref.shape[1] // tile):
        cols = slice(j * tile, (j + 1) * tile)
        t = jnp.dot(h, wup_ref[:, cols], preferred_element_type=F32) + bup_ref[:, cols]
        t2 = t * t
        th = jnp.tanh(t * (GELU_A + (GELU_A * GELU_B) * t2))
        half_t = 0.5 * t
        act = (half_t + half_t * th).astype(BF16)
        act_ref[:, cols] = act
        act_all_ref[:, cols] = act
        slope_ref[:, cols] = 0.5 + 0.5 * th + half_t * (1.0 - th * th) * (GELU_A + (3 * GELU_A * GELU_B) * t2)
    n = qkv_ref.shape[1]
    for j in range(0, n, tile):
        cols = slice(j, min(j + tile, n))
        qkv_ref[:, cols] = (jnp.dot(h, wqkv_ref[:, cols], preferred_element_type=F32) + bqkv_ref[:, cols]).astype(BF16)


def front_h(h, w_qkv, b_qkv, w_up, b_up, row0, total, full, bm=512, tile=256):
    rows, d = h.shape
    n1, n2 = w_qkv.shape[1], w_up.shape[1]
    blk = lambda c: pl.BlockSpec((bm, c), lambda i: (i, 0))
    off = lambda c: pl.BlockSpec((bm, c), lambda i: (i + row0 // bm, 0))
    return call(functools.partial(front_h_kernel, tile), "front_h", (rows // bm,),
                [(h, blk(d)), const(w_qkv), const(b_qkv), const(w_up), const(b_up)],
                [((rows, n1), BF16, blk(n1)), ((rows, n2), BF16, blk(n2)), ((rows, n2), F32, blk(n2)),
                 ((total, n2), BF16, off(n2)), ((total, d), BF16, off(d))], 2 * rows * d * (n1 + n2), full)


def front_d_kernel(tile, dy_ref, wo_ref, wdown_ref, slope_ref, dctx_ref, dpre_ref, bsum_ref, dpre_all_ref, dy_all_ref):
    @pl.when(pl.program_id(0) == 0)
    def _():
        bsum_ref[...] = jnp.zeros_like(bsum_ref)

    dy = dy_ref[...]
    dy_all_ref[...] = dy
    for j in range(dpre_ref.shape[1] // tile):
        cols = slice(j * tile, (j + 1) * tile)
        d_pre = dot_t(dy, wdown_ref[cols, :], ((1,), (1,))) * slope_ref[:, cols]
        bsum_ref[:, cols] += jnp.sum(d_pre, axis=0, keepdims=True)
        dpre_ref[:, cols] = d_pre.astype(BF16)
        dpre_all_ref[:, cols] = d_pre.astype(BF16)
    dctx_ref[...] = dot_t(dy, wo_ref[...], ((1,), (1,))).astype(BF16)


def front_d(dy, w_o, w_down, slope, row0, total, full, bm=512, tile=256):
    rows, d = dy.shape
    n1, n2 = w_o.shape[0], w_down.shape[0]
    blk = lambda c: pl.BlockSpec((bm, c), lambda i: (i, 0))
    off = lambda c: pl.BlockSpec((bm, c), lambda i: (i + row0 // bm, 0))
    return call(functools.partial(front_d_kernel, tile), "front_d", (rows // bm,),
                [(dy, blk(d)), const(w_o), const(w_down), (slope, blk(n2))],
                [((rows, n1), BF16, blk(n1)), ((rows, n2), BF16, blk(n2)),
                 ((1, n2), F32, pl.BlockSpec((1, n2), lambda i: (0, 0))),
                 ((total, n2), BF16, off(n2)), ((total, d), BF16, off(d))], 2 * rows * d * (n1 + n2), full)


def pair_kernel(tile, a_ref, b_ref, wa_ref, wb_ref, out_ref):
    for j in range(out_ref.shape[1] // tile):
        cols = slice(j * tile, (j + 1) * tile)
        out_ref[:, cols] = (jnp.dot(a_ref[...], wa_ref[:, cols], preferred_element_type=F32)
                            + jnp.dot(b_ref[...], wb_ref[:, cols], preferred_element_type=F32)).astype(BF16)


def pair_matmul(a, b, wa, wb, name, bm=512, tile=256):
    rows, ka = a.shape
    kb, n = wb.shape
    blk = lambda c: pl.BlockSpec((bm, c), lambda i: (i, 0))
    return call(functools.partial(pair_kernel, tile), name, (rows // bm,),
                [(a, blk(ka)), (b, blk(kb)), const(wa), const(wb)], [((rows, n), BF16, blk(n))],
                2 * rows * (ka + kb) * n)[0]


def layer_body(x_blk, rope_angle, ln_gain, ln_bias, w_q, b_q, w_k, b_k, w_v, b_v, w_o, b_o, w_up, b_up, w_down, b_down, dy_blk):
    n_seq, s_loc, model_dim = x_blk.shape
    seq_len, half_rot = rope_angle.shape
    heads, head_dim = b_q.shape
    width = heads * head_dim
    total = n_seq * seq_len

    pad = head_dim - 2 * half_rot
    cos_full = jnp.concatenate([jnp.cos(rope_angle)] * 2 + [jnp.ones((seq_len, pad), F32)], axis=-1)
    sin_full = jnp.concatenate([jnp.sin(rope_angle)] * 2 + [jnp.zeros((seq_len, pad), F32)], axis=-1)
    w_qkv = jnp.concatenate([w_q, w_k, w_v], axis=1)
    b_qkv = jnp.concatenate([b_q.reshape(1, -1), b_k.reshape(1, -1), b_v.reshape(1, -1)], axis=1)
    w_qkv_t, w_up_t = w_qkv.T, w_up.T

    edges = [0]
    for part in CHUNK_PARTS:
        edges.append(edges[-1] + n_seq * part // sum(CHUNK_PARTS))
    chunks = [slice(a, b) for a, b in zip(edges[:-1], edges[1:])]
    row3 = lambda off=0: pl.BlockSpec((1, s_loc, model_dim), lambda i: (i + off, 0, 0))
    gain, bias, bo, bdown = (t.reshape(1, -1) for t in (ln_gain, ln_bias, b_o, b_down))
    h_full, dy_full = [], []
    for sl in chunks:
        n = sl.stop - sl.start
        h_loc = call(ln_fwd_kernel, "ln_fwd", (n,), [(x_blk, row3(sl.start)), const(gain), const(bias)],
                     [((n, s_loc, model_dim), BF16, row3())], n * s_loc * model_dim * 200)[0]
        h_full.append(lax.all_gather(h_loc, 'tp', axis=1, tiled=True))
        dy_full.append(lax.all_gather(dy_blk[sl], 'tp', axis=1, tiled=True))

    bsum, bup_sum, small = 0, 0, 0
    y_all = dx_all = None
    act_all = h_all = dpre_all = dy_all = ctx_all = dqkv_all = None
    tie = None
    for c, sl in enumerate(chunks):
        per = sl.stop - sl.start
        rows, row0 = per * seq_len, sl.start * seq_len
        h, dy = h_full[c].reshape(rows, model_dim), dy_full[c].reshape(rows, model_dim)
        if tie is not None:
            h, tie = lax.optimization_barrier((h, tie))
        qkv, act, slope, act_all, h_all = front_h(h, w_qkv, b_qkv, w_up, b_up.reshape(1, -1), row0, total, (act_all, h_all))
        d_ctx, d_pre, b_part, dpre_all, dy_all = front_d(dy, w_o, w_down, slope, row0, total, (dpre_all, dy_all))
        bup_sum += b_part[0]
        ctx, d_qkv, b_part, ctx_all, dqkv_all = attention(
            qkv.reshape(per, seq_len, 3 * width), d_ctx.reshape(per, seq_len, width), cos_full, sin_full,
            heads, head_dim, half_rot, sl.start, total, (ctx_all, dqkv_all))
        bsum += b_part[0]
        ctx, d_qkv = ctx.reshape(rows, width), d_qkv.reshape(rows, 3 * width)
        branch = pair_matmul(ctx, act, w_o, w_down, "branch")
        d_qkv, branch = lax.optimization_barrier((d_qkv, branch))
        d_h = pair_matmul(d_qkv, d_pre, w_qkv_t, w_up_t, "d_h")
        tie = d_h
        branch_sum = lax.psum_scatter(branch.reshape(per, seq_len, model_dim), 'tp', scatter_dimension=1, tiled=True)
        y_all = call(residual_kernel, "residual", (per,), [(x_blk, row3(sl.start)), (branch_sum, row3()), const(bo), const(bdown)],
                     [((n_seq, s_loc, model_dim), BF16, row3(sl.start))], per * s_loc * model_dim * 100, (y_all,))[0]
        d_h_loc = lax.psum_scatter(d_h.reshape(per, seq_len, model_dim), 'tp', scatter_dimension=1, tiled=True)
        d_h_loc, y_all = lax.optimization_barrier((d_h_loc, y_all))
        part, dx_all = call(ln_bwd_kernel, "ln_bwd", (per,),
                            [(x_blk, row3(sl.start)), (dy_blk, row3(sl.start)), (d_h_loc, row3()), const(gain)],
                            [((8, model_dim), F32, pl.BlockSpec((8, model_dim), lambda i: (0, 0))),
                             ((n_seq, s_loc, model_dim), F32, row3(sl.start))], per * s_loc * model_dim * 200, (dx_all,))
        small += part[:3]
    h_all, dy_all, act_all, ctx_all, tie = lax.optimization_barrier((h_all, dy_all, act_all, ctx_all, tie))
    t0 = ((0,), (0,))
    g_o = dot_t(ctx_all, dy_all, t0)
    g_down = dot_t(act_all, dy_all, t0)
    g_qkv = dot_t(h_all, dqkv_all, t0)
    g_up = dot_t(h_all, dpre_all, t0)
    small = lax.psum(small, 'tp')
    bsum = bsum.reshape(3, heads, head_dim)
    return (y_all, dx_all, small[0], small[1],
            g_qkv[:, :width], bsum[0], g_qkv[:, width:2 * width], bsum[1], g_qkv[:, 2 * width:], bsum[2],
            g_o, small[2], g_up, bup_sum, g_down, small[2])


def solution(mesh):
    row_spec = P('dp', 'tp', None)
    col_spec = P(None, 'tp')
    head_spec = P('tp', None)
    grad_cols = P('dp', 'tp')
    grad_rows = P(('dp', 'tp'), None)
    in_specs = (row_spec, P(None, None), P(None), P(None), col_spec, head_spec, col_spec, head_spec,
                col_spec, head_spec, P('tp', None), P(None), col_spec, P('tp'), P('tp', None), P(None), row_spec)
    out_specs = (row_spec, row_spec, P('dp'), P('dp'), grad_cols, grad_rows, grad_cols, grad_rows, grad_cols,
                 grad_rows, grad_rows, P('dp'), grad_cols, P(('dp', 'tp')), grad_rows, P('dp'))
    return jax.shard_map(layer_body, mesh=mesh, in_specs=in_specs, out_specs=out_specs, check_vma=False)
```

```python
import functools

import jax
import jax.numpy as jnp
from jax import lax
from jax.experimental import pallas as pl
from jax.experimental.pallas import tpu as pltpu
from jax.sharding import PartitionSpec as P

LN_EPS = 1e-5
CHUNK_PARTS = (3, 5, 8)
LOG2E = 1.4426950408889634
GELU_A, GELU_B = 0.7978845608028654, 0.044715
F32, BF16 = jnp.float32, jnp.bfloat16


def dot_t(a, b, dims):
    return lax.dot_general(a, b, (dims, ((), ())), preferred_element_type=F32)


def call(kernel, name, grid, ins, outs, flops, full=()):
    arrays, specs = [a for a, _ in ins], [s for _, s in ins]
    first = len(outs) - len(full)
    aliases = {}
    for i, prev in enumerate(full):
        if prev is not None:
            aliases[len(arrays)] = first + i
            arrays.append(prev)
            specs.append(pl.BlockSpec(memory_space=pl.ANY))
    n_in = len(ins)

    def body(*refs):
        kernel(*refs[:n_in], *refs[len(arrays):])

    moved = sum(a.size * a.dtype.itemsize for a, _ in ins)
    return pl.pallas_call(
        body, grid=grid, in_specs=specs, out_specs=[s for _, _, s in outs],
        out_shape=[jax.ShapeDtypeStruct(s, d) for s, d, _ in outs], input_output_aliases=aliases,
        cost_estimate=pl.CostEstimate(flops=flops, bytes_accessed=moved, transcendentals=0), name=name)(*arrays)


def attn_kernel(heads, head_dim, half_rot, qkv_ref, dctx_ref, cos_ref, sin_ref, ctx_ref, dqkv_ref, bsum_ref, ctx_all_ref, dqkv_all_ref):
    seq_len = qkv_ref.shape[1]
    half = seq_len // 2
    width = heads * head_dim
    scale = head_dim ** -0.5
    cos_t, sin_t = cos_ref[...], sin_ref[...]
    mask = (lax.broadcasted_iota(jnp.int32, (half, half), 0) <= lax.broadcasted_iota(jnp.int32, (half, half), 1))

    def rope(t, sin_s):
        turned = jnp.concatenate([-t[:, half_rot:2 * half_rot], t[:, :half_rot], t[:, 2 * half_rot:]], axis=-1)
        return t * cos_t + turned * sin_s

    @pl.when(pl.program_id(0) == 0)
    def _():
        bsum_ref[...] = jnp.zeros_like(bsum_ref)

    units = [(i, b) for i in range(heads) for b in range(2)]
    loaded, scored, soft, acc = {}, {}, {}, {}

    def head_cols(i):
        return [slice(w * width + i * head_dim, w * width + (i + 1) * head_dim) for w in range(3)]

    def load_head(i):
        cols = head_cols(i)
        q = rope(qkv_ref[0, :, cols[0]].astype(F32), sin_t).astype(BF16)
        k = rope(qkv_ref[0, :, cols[1]].astype(F32), sin_t).astype(BF16)
        v = qkv_ref[0, :, cols[2]]
        loaded[i] = (q, k, v, dctx_ref[0, :, cols[0]], k.T, v.T)

    def score(i, b):
        if b == 0:
            load_head(i)
        q, k, v, d_ctx, _, _ = loaded[i]
        rows, keys = slice(b * half, (b + 1) * half), (b + 1) * half
        scored[i, b] = (dot_t(k[:keys], q[rows], ((1,), (1,))), dot_t(v[:keys], d_ctx[rows], ((1,), (1,))))

    def softmax(i, b):
        s, d_prob = scored.pop((i, b))
        diag = jnp.where(mask, s[b * half:], -1e30)
        s = diag if b == 0 else jnp.concatenate([s[:half], diag], axis=0)
        e = jnp.exp2((s - jnp.max(s, axis=0, keepdims=True)) * (scale * LOG2E))
        prob = e * (1.0 / jnp.sum(e, axis=0, keepdims=True))
        d_score = (prob * (d_prob - jnp.sum(d_prob * prob, axis=0, keepdims=True)) * scale).astype(BF16)
        soft[i, b] = (prob.astype(BF16), d_score)

    def products(i, b):
        prob_bf, d_score = soft.pop((i, b))
        q, k, v, d_ctx, k_t, v_t = loaded[i]
        rows, keys = slice(b * half, (b + 1) * half), (b + 1) * half
        acc[b] = (dot_t(v_t[:, :keys], prob_bf, ((1,), (0,))).astype(BF16), dot_t(k_t[:, :keys], d_score, ((1,), (0,))),
                  dot_t(d_score, q[rows], ((1,), (0,))), dot_t(prob_bf, d_ctx[rows], ((1,), (0,))))
        if b == 0:
            return
        cols = head_cols(i)
        ctx = jnp.concatenate([acc[0][0], acc[1][0]], axis=1).T
        ctx_ref[0, :, cols[0]] = ctx
        ctx_all_ref[:, cols[0]] = ctx
        d_q = rope(jnp.concatenate([acc[0][1], acc[1][1]], axis=1).T, -sin_t)
        d_k = rope(jnp.concatenate([acc[0][2] + acc[1][2][:half], acc[1][2][half:]], axis=0), -sin_t)
        d_v = jnp.concatenate([acc[0][3] + acc[1][3][:half], acc[1][3][half:]], axis=0)
        for d_p, col in zip((d_q, d_k, d_v), cols):
            dqkv_ref[0, :, col] = d_p.astype(BF16)
            dqkv_all_ref[:, col] = d_p.astype(BF16)
            bsum_ref[:, col] += jnp.sum(d_p, axis=0, keepdims=True)

    for n in range(len(units) + 2):
        if n < len(units):
            score(*units[n])
        if 1 <= n <= len(units):
            softmax(*units[n - 1])
        if n >= 2:
            products(*units[n - 2])


def attention(qkv, d_ctx, cos_full, sin_full, heads, head_dim, half_rot, seq0, total, full):
    n_seq, seq_len, width3 = qkv.shape
    width = heads * head_dim
    tab = pl.BlockSpec((seq_len, head_dim), lambda i: (0, 0))
    block = lambda w: pl.BlockSpec((1, seq_len, w), lambda i: (i, 0, 0))
    rows = lambda w: pl.BlockSpec((seq_len, w), lambda i: (i + seq0, 0))
    return call(functools.partial(attn_kernel, heads, head_dim, half_rot), "attention", (n_seq,),
                [(qkv, block(width3)), (d_ctx, block(width)), (cos_full, tab), (sin_full, tab)],
                [((n_seq, seq_len, width), BF16, block(width)), ((n_seq, seq_len, width3), BF16, block(width3)),
                 ((1, width3), F32, pl.BlockSpec((1, width3), lambda i: (0, 0))),
                 ((total, width), BF16, rows(width)), ((total, width3), BF16, rows(width3))],
                n_seq * heads * 4 * 2 * seq_len * seq_len * 256, full)


def const(arr):
    return (arr, pl.BlockSpec(arr.shape, lambda i: (0, 0)))


def normalize(x):
    x_f = x.astype(F32)
    centered = x_f - jnp.mean(x_f, axis=-1, keepdims=True)
    inv_std = lax.rsqrt(jnp.mean(centered * centered, axis=-1, keepdims=True) + LN_EPS)
    return centered * inv_std, inv_std


def ln_fwd_kernel(x_ref, gain_ref, bias_ref, h_ref):
    normed, _ = normalize(x_ref[0])
    h_ref[0] = (normed * gain_ref[...] + bias_ref[...]).astype(BF16)


def ln_bwd_kernel(x_ref, dy_ref, dh_ref, gain_ref, sums_ref, dx_ref):
    @pl.when(pl.program_id(0) == 0)
    def _():
        sums_ref[...] = jnp.zeros_like(sums_ref)

    normed, inv_std = normalize(x_ref[0])
    d_h, dy = dh_ref[0].astype(F32), dy_ref[0].astype(F32)
    d_norm = d_h * gain_ref[...]
    sums_ref[0:1] += jnp.sum(d_h * normed, axis=0, keepdims=True)
    sums_ref[1:2] += jnp.sum(d_h, axis=0, keepdims=True)
    sums_ref[2:3] += jnp.sum(dy, axis=0, keepdims=True)
    dx_ref[0] = dy + inv_std * (d_norm - jnp.mean(d_norm, axis=-1, keepdims=True)
                                - normed * jnp.mean(d_norm * normed, axis=-1, keepdims=True))


def residual_kernel(x_ref, part_ref, bo_ref, bdown_ref, y_ref):
    y_ref[0] = (x_ref[0].astype(F32) + part_ref[0].astype(F32) + bo_ref[...] + bdown_ref[...]).astype(BF16)


def front_h_kernel(tile, h_ref, wqkv_ref, bqkv_ref, wup_ref, bup_ref, qkv_ref, act_ref, slope_ref, act_all_ref, h_all_ref):
    h_all_ref[...] = h_ref[...]
    n_up, n_qkv = act_ref.shape[1], qkv_ref.shape[1]
    jobs = []
    ups = [('u', slice(j, j + tile)) for j in range(0, n_up, tile)]
    qs = [('q', slice(j, min(j + tile, n_qkv))) for j in range(0, n_qkv, tile)]
    while ups or qs:
        jobs += [rest.pop(0) for rest in (ups, qs) if rest]

    def product(kind, cols):
        if kind == 'u':
            return jnp.dot(h_ref[...], wup_ref[:, cols], preferred_element_type=F32)
        return dot_t(h_ref[...], wqkv_ref[cols, :], ((1,), (1,)))

    def finish(kind, cols, t):
        if kind == 'q':
            qkv_ref[:, cols] = (t + bqkv_ref[:, cols]).astype(BF16)
            return
        t = t + bup_ref[:, cols]
        t2 = t * t
        th = jnp.tanh(t * (GELU_A + (GELU_A * GELU_B) * t2))
        half_t = 0.5 * t
        act = (half_t + half_t * th).astype(BF16)
        act_ref[:, cols] = act
        act_all_ref[:, cols] = act
        slope_ref[:, cols] = 0.5 + 0.5 * th + half_t * (1.0 - th * th) * (GELU_A + (3 * GELU_A * GELU_B) * t2)

    prev = None
    for job in jobs:
        t = product(*job)
        if prev is not None:
            finish(*prev)
        prev = (*job, t)
    finish(*prev)


def front_h(h, w_qkv_t, b_qkv, w_up, b_up, row0, total, full, bm=256, tile=256):
    rows, d = h.shape
    n1, n2 = w_qkv_t.shape[0], w_up.shape[1]
    blk = lambda c: pl.BlockSpec((bm, c), lambda i: (i, 0))
    off = lambda c: pl.BlockSpec((bm, c), lambda i: (i + row0 // bm, 0))
    return call(functools.partial(front_h_kernel, tile), "front_h", (rows // bm,),
                [(h, blk(d)), const(w_qkv_t), const(b_qkv), const(w_up), const(b_up)],
                [((rows, n1), BF16, blk(n1)), ((rows, n2), BF16, blk(n2)), ((rows, n2), F32, blk(n2)),
                 ((total, n2), BF16, off(n2)), ((total, d), BF16, off(d))], 2 * rows * d * (n1 + n2), full)


def front_d_kernel(tile, dy_ref, wo_ref, wdown_ref, slope_ref, dctx_ref, dpre_ref, bsum_ref, dpre_all_ref, dy_all_ref):
    @pl.when(pl.program_id(0) == 0)
    def _():
        bsum_ref[...] = jnp.zeros_like(bsum_ref)

    dy = dy_ref[...]
    dy_all_ref[...] = dy
    for j in range(dpre_ref.shape[1] // tile):
        cols = slice(j * tile, (j + 1) * tile)
        d_pre = dot_t(dy, wdown_ref[cols, :], ((1,), (1,))) * slope_ref[:, cols]
        bsum_ref[:, cols] += jnp.sum(d_pre, axis=0, keepdims=True)
        dpre_ref[:, cols] = d_pre.astype(BF16)
        dpre_all_ref[:, cols] = d_pre.astype(BF16)
    dctx_ref[...] = dot_t(dy, wo_ref[...], ((1,), (1,))).astype(BF16)


def front_d(dy, w_o, w_down, slope, row0, total, full, bm=512, tile=256):
    rows, d = dy.shape
    n1, n2 = w_o.shape[0], w_down.shape[0]
    blk = lambda c: pl.BlockSpec((bm, c), lambda i: (i, 0))
    off = lambda c: pl.BlockSpec((bm, c), lambda i: (i + row0 // bm, 0))
    return call(functools.partial(front_d_kernel, tile), "front_d", (rows // bm,),
                [(dy, blk(d)), const(w_o), const(w_down), (slope, blk(n2))],
                [((rows, n1), BF16, blk(n1)), ((rows, n2), BF16, blk(n2)),
                 ((1, n2), F32, pl.BlockSpec((1, n2), lambda i: (0, 0))),
                 ((total, n2), BF16, off(n2)), ((total, d), BF16, off(d))], 2 * rows * d * (n1 + n2), full)


def pair_kernel(tile, b_dim, a_ref, b_ref, wa_ref, wb_ref, out_ref):
    for j in range(out_ref.shape[1] // tile):
        cols = slice(j * tile, (j + 1) * tile)
        wb = wb_ref[:, cols] if b_dim == 0 else wb_ref[cols, :]
        out_ref[:, cols] = (jnp.dot(a_ref[...], wa_ref[:, cols], preferred_element_type=F32)
                            + dot_t(b_ref[...], wb, ((1,), (b_dim,)))).astype(BF16)


def pair_matmul(a, b, wa, wb, name, b_dim=0, bm=512, tile=256, splits=2):
    rows, ka = a.shape
    kb, n = b.shape[1], wa.shape[1]
    bn = n // splits
    lhs = lambda c: pl.BlockSpec((bm, c), lambda j, i: (i, 0))
    wb_spec = pl.BlockSpec((kb, bn), lambda j, i: (0, j)) if b_dim == 0 else pl.BlockSpec((bn, kb), lambda j, i: (j, 0))
    return call(functools.partial(pair_kernel, tile, b_dim), name, (splits, rows // bm),
                [(a, lhs(ka)), (b, lhs(kb)), (wa, pl.BlockSpec((ka, bn), lambda j, i: (0, j))), (wb, wb_spec)],
                [((rows, n), BF16, pl.BlockSpec((bm, bn), lambda j, i: (i, j)))], 2 * rows * (ka + kb) * n)[0]


def sum_over_tp(t):
    n, step = lax.axis_size('tp'), 1
    while step < n:
        t = t + lax.ppermute(t, 'tp', [(i, i ^ step) for i in range(n)])
        step *= 2
    return t


def layer_body(x_blk, rope_angle, ln_gain, ln_bias, w_q, b_q, w_k, b_k, w_v, b_v, w_o, b_o, w_up, b_up, w_down, b_down, dy_blk):
    n_seq, s_loc, model_dim = x_blk.shape
    seq_len, half_rot = rope_angle.shape
    heads, head_dim = b_q.shape
    width = heads * head_dim
    total = n_seq * seq_len

    pad = head_dim - 2 * half_rot
    cos_full = jnp.concatenate([jnp.cos(rope_angle)] * 2 + [jnp.ones((seq_len, pad), F32)], axis=-1)
    sin_full = jnp.concatenate([jnp.sin(rope_angle)] * 2 + [jnp.zeros((seq_len, pad), F32)], axis=-1)
    w_qkv_t = jnp.concatenate([w_q.T, w_k.T, w_v.T], axis=0)
    b_qkv = jnp.concatenate([b_q.reshape(1, -1), b_k.reshape(1, -1), b_v.reshape(1, -1)], axis=1)

    edges = [0]
    for part in CHUNK_PARTS:
        edges.append(edges[-1] + n_seq * part // sum(CHUNK_PARTS))
    chunks = [slice(a, b) for a, b in zip(edges[:-1], edges[1:])]
    row3 = lambda off=0: pl.BlockSpec((1, s_loc, model_dim), lambda i: (i + off, 0, 0))
    gain, bias, bo, bdown = (t.reshape(1, -1) for t in (ln_gain, ln_bias, b_o, b_down))
    h_full, dy_full = [], []
    for sl in chunks:
        n = sl.stop - sl.start
        h_loc = call(ln_fwd_kernel, "ln_fwd", (n,), [(x_blk, row3(sl.start)), const(gain), const(bias)],
                     [((n, s_loc, model_dim), BF16, row3())], n * s_loc * model_dim * 200)[0]
        h_full.append(lax.all_gather(h_loc, 'tp', axis=1, tiled=True))
        dy_full.append(lax.all_gather(dy_blk[sl], 'tp', axis=1, tiled=True))

    bsum, bup_sum, small = 0, 0, 0
    y_all = dx_all = None
    act_all = h_all = dpre_all = dy_all = ctx_all = dqkv_all = None
    tie = None
    for c, sl in enumerate(chunks):
        per = sl.stop - sl.start
        rows, row0 = per * seq_len, sl.start * seq_len
        h, dy = h_full[c].reshape(rows, model_dim), dy_full[c].reshape(rows, model_dim)
        if tie is not None:
            h, tie = lax.optimization_barrier((h, tie))
        qkv, act, slope, act_all, h_all = front_h(h, w_qkv_t, b_qkv, w_up, b_up.reshape(1, -1), row0, total, (act_all, h_all))
        d_ctx, d_pre, b_part, dpre_all, dy_all = front_d(dy, w_o, w_down, slope, row0, total, (dpre_all, dy_all))
        bup_sum += b_part[0]
        ctx, d_qkv, b_part, ctx_all, dqkv_all = attention(
            qkv.reshape(per, seq_len, 3 * width), d_ctx.reshape(per, seq_len, width), cos_full, sin_full,
            heads, head_dim, half_rot, sl.start, total, (ctx_all, dqkv_all))
        bsum += b_part[0]
        ctx, d_qkv = ctx.reshape(rows, width), d_qkv.reshape(rows, 3 * width)
        branch = pair_matmul(ctx, act, w_o, w_down, "branch")
        d_qkv, branch = lax.optimization_barrier((d_qkv, branch))
        d_h = pair_matmul(d_qkv, d_pre, w_qkv_t, w_up, "d_h", b_dim=1)
        tie = d_h
        branch_sum = lax.psum_scatter(branch.reshape(per, seq_len, model_dim), 'tp', scatter_dimension=1, tiled=True)
        y_all = call(residual_kernel, "residual", (per,), [(x_blk, row3(sl.start)), (branch_sum, row3()), const(bo), const(bdown)],
                     [((n_seq, s_loc, model_dim), BF16, row3(sl.start))], per * s_loc * model_dim * 100, (y_all,))[0]
        d_h_loc = lax.psum_scatter(d_h.reshape(per, seq_len, model_dim), 'tp', scatter_dimension=1, tiled=True)
        d_h_loc, y_all = lax.optimization_barrier((d_h_loc, y_all))
        part, dx_all = call(ln_bwd_kernel, "ln_bwd", (per,),
                            [(x_blk, row3(sl.start)), (dy_blk, row3(sl.start)), (d_h_loc, row3()), const(gain)],
                            [((8, model_dim), F32, pl.BlockSpec((8, model_dim), lambda i: (0, 0))),
                             ((n_seq, s_loc, model_dim), F32, row3(sl.start))], per * s_loc * model_dim * 200, (dx_all,))
        small += part[:3]
    h_all, dy_all, act_all, ctx_all, tie = lax.optimization_barrier((h_all, dy_all, act_all, ctx_all, tie))
    t0 = ((0,), (0,))
    g_o = dot_t(ctx_all, dy_all, t0)
    g_down = dot_t(act_all, dy_all, t0)
    g_qkv = dot_t(h_all, dqkv_all, t0)
    g_up = dot_t(h_all, dpre_all, t0)
    small = sum_over_tp(small)
    bsum = bsum.reshape(3, heads, head_dim)
    return (y_all, dx_all, small[0], small[1],
            g_qkv[:, :width], bsum[0], g_qkv[:, width:2 * width], bsum[1], g_qkv[:, 2 * width:], bsum[2],
            g_o, small[2], g_up, bup_sum, g_down, small[2])


def solution(mesh):
    row_spec = P('dp', 'tp', None)
    col_spec = P(None, 'tp')
    head_spec = P('tp', None)
    grad_cols = P('dp', 'tp')
    grad_rows = P(('dp', 'tp'), None)
    in_specs = (row_spec, P(None, None), P(None), P(None), col_spec, head_spec, col_spec, head_spec,
                col_spec, head_spec, P('tp', None), P(None), col_spec, P('tp'), P('tp', None), P(None), row_spec)
    out_specs = (row_spec, row_spec, P('dp'), P('dp'), grad_cols, grad_rows, grad_cols, grad_rows, grad_cols,
                 grad_rows, grad_rows, P('dp'), grad_cols, P(('dp', 'tp')), grad_rows, P('dp'))
    return jax.shard_map(layer_body, mesh=mesh, in_specs=in_specs, out_specs=out_specs, check_vma=False)
```
